32 devices in a mesh: dom: 16 (over z, y, core), sub: 2 (over x).
Axes of the slice: x: 2, y: 2, z: 4, core: 2. Of those that a mesh axis runs over, the one named last changes fastest.
Arguments:
- solution: float32 [125, 5, 1024], P(None, None, ('dom', 'sub')), may hold values from -1.2 to 5.4, as said below
- face_link: int32 [6, 1024], P(None, ('dom', 'sub')), may hold values from 0 to 6143, as said below
Outputs:
- rate: float32 [125, 5, 1024], P(None, None, ('dom', 'sub'))
The draws below stay inside these ranges and needn't reach their ends.
Inputs may be any that keep to these rules, and one draw needn't show every extreme that they name: At every solution point density lies between 0.6 and 1.4, each velocity component between -0.8 and 0.8 and pressure between 0.6 and 1.6; at every flux point the interpolated density and pressure stay at 0.5 or more and each interpolated velocity component between -1.1 and 1.1. `face_link`: the pairing is mutual and pairs face 2 a + 1 of one element with face 2 a of another, point for point. Elements are numbered device by device in the order of the joined axes, 32 to a device; a partner lies in the same partition or in one whose dom index differs by at most 2 cyclically. At most 6 faces of one device pair with faces of any one other device, and in every draw some pair of devices reaches 6.
All inputs are finite; a program needn't handle non-finite values.
Results may differ from the reference program's by a relative error of at most 0.0003.
Values sent between devices are 32-bit elements; how exact they have to be, the bound alone decides.
No kernel may reach another device: no remote copies, remote signals or barrier semaphores. Data moves between devices by JAX's collectives and lax.ppermute only.
A program may use at most 64 MiB of HBM per device.

```python
import jax
import jax.numpy as jnp
import numpy as np
from jax import lax

ORDER = 4
NSIDE = 5
NPTS = 125
ELEM_DEV = 32
CAP = 6
ELEMS = 1024
N_DOM = 16
N_SUB = 2


heat_ratio = 1.4


def point_coordinates():
    point_ids = jnp.arange(NPTS, dtype=jnp.int32)
    index_list = [point_ids // (NSIDE * NSIDE), point_ids // NSIDE % NSIDE, point_ids % NSIDE]
    half_span = 0.5 * (NSIDE - 1)
    return jnp.stack([(member.astype(jnp.float32) - half_span) / half_span for member in index_list])


def smooth_field(key, count, mean_lo, mean_hi, slope_amp, noise_amp):
    key_mean, key_slope, key_noise = jax.random.split(key, 3)
    coords = point_coordinates()
    means = jax.random.uniform(key_mean, (count, 1, ELEMS), jnp.float32, mean_lo, mean_hi)
    slopes = jax.random.uniform(key_slope, (count, 3, ELEMS), jnp.float32, -slope_amp, slope_amp)
    linear = jnp.einsum('cae,ap->cpe', slopes, coords)
    noise = jax.random.uniform(key_noise, (count, NPTS, ELEMS), jnp.float32, -noise_amp, noise_amp)
    return means + linear + noise


def draw_solution(key, part):
    subkeys = jax.random.split(key, 3)
    density = smooth_field(subkeys[0], 1, 0.9, 1.1, 0.03, 0.04)[0]
    mean_flow = jnp.array([0.2, 0.0, -0.1], jnp.float32).reshape(3, 1, 1)
    velocity = mean_flow + smooth_field(subkeys[1], 3, -0.2, 0.2, 0.05, 0.08)
    pressure = smooth_field(subkeys[2], 1, 0.9, 1.1, 0.03, 0.04)[0]
    energy = pressure / (heat_ratio - 1.0) + 0.5 * density * jnp.sum(velocity * velocity, axis=0)
    momentum = density[None] * velocity
    return jnp.stack([density, momentum[0], momentum[1], momentum[2], energy], axis=1).astype(jnp.float32)


def draw_face_link(key, part):
    devices = N_DOM * N_SUB
    dev_ids = jnp.arange(devices, dtype=jnp.int32)
    dom_ids = dev_ids // N_SUB
    sub_ids = dev_ids % N_SUB
    classes = jnp.arange(N_SUB, dtype=jnp.int32)
    slots = jnp.arange(ELEM_DEV, dtype=jnp.int32)
    pick_pair, pick_far = jax.random.split(jax.random.fold_in(key, 101))
    star_pair = jax.random.randint(pick_pair, (), 1, N_SUB)
    star_far = jax.random.randint(pick_far, (), 0, N_SUB)
    ceilings = (CAP - 2 * (CAP // 3), CAP // 3, CAP // 3)
    link_table = jnp.zeros((6, devices, ELEM_DEV), jnp.int32)
    for direction in range(3):
        ceiling = ceilings[direction]
        half_cap = ceiling // 2
        key_pair, key_far, key_near, key_slot, key_elem = jax.random.split(jax.random.fold_in(key, direction), 5)
        pairs = jax.random.randint(key_pair, (N_SUB,), 0, half_cap + 1)
        pairs = jnp.where((classes == star_pair) | (classes == (N_SUB - star_pair) % N_SUB), half_cap, pairs)
        pairs = jnp.where(classes == 0, 0, pairs)
        remote = jax.random.randint(key_far, (N_SUB,), ceiling, 2 * ceiling + 1)
        remote = jnp.where(classes == star_far, 2 * ceiling, remote)
        block_sizes = jnp.concatenate([pairs, remote])
        block_ends = jnp.cumsum(block_sizes)
        block_starts = block_ends - block_sizes
        block_of = jnp.sum((slots[:, None] >= block_ends[None, :]).astype(jnp.int32), axis=1)
        inside = block_of < 2 * N_SUB
        clamped = jnp.minimum(block_of, 2 * N_SUB - 1)
        shift_sub = jnp.where(inside, clamped % N_SUB, 0)
        offset_in = slots - block_starts[clamped]
        near_count = jax.random.randint(key_near, (N_SUB, N_SUB), remote[None, :] - ceiling, ceiling + 1)
        far_block = inside & (block_of >= N_SUB)
        near_at = near_count[:, shift_sub]
        hops = jnp.where(far_block[None, :], jnp.where(offset_in[None, :] < near_at, 1, 2), 0)
        reorder = jax.random.permutation(key_slot, ELEM_DEV)
        shift_sub = shift_sub[reorder]
        hops = hops[:, reorder]
        members = jax.vmap(lambda elem_key: jax.random.permutation(elem_key, ELEM_DEV))(jax.random.split(key_elem, devices)).astype(jnp.int32)
        dest_dom = (dom_ids[:, None] + hops[sub_ids]) % N_DOM
        dest_sub = (sub_ids[:, None] + shift_sub[None, :]) % N_SUB
        dest_dev = dest_dom * N_SUB + dest_sub
        dest_elem = members[dest_dev, slots[None, :]]
        own_global = dev_ids[:, None] * ELEM_DEV + members
        dest_global = dest_dev * ELEM_DEV + dest_elem
        link_table = link_table.at[2 * direction + 1, dev_ids[:, None], members].set(dest_global * 6 + 2 * direction)
        link_table = link_table.at[2 * direction, dest_dev, dest_elem].set(own_global * 6 + 2 * direction + 1)
    return link_table.reshape(6, devices * ELEM_DEV)


def setup_inputs(seed: int = 0) -> dict:
    arg_keys = jax.random.split(jax.random.key(seed), 3)
    solution = draw_solution(jax.random.fold_in(arg_keys[2], 71), 0)
    face_link = draw_face_link(jax.random.fold_in(arg_keys[2], 71), 0)
    return {"solution": solution, "face_link": face_link}


heat_ratio = 1.4
viscosity = 0.08
prandtl = 0.72
penalty = 0.1

def legendre_table(degree, abscissae):
    values = [abscissae * 0.0 + 1.0, abscissae.copy()]
    slopes = [abscissae * 0.0, abscissae * 0.0 + 1.0]
    for current in range(1, degree):
        values.append(((2 * current + 1) * abscissae * values[current] - current * values[current - 1]) / (current + 1))
        slopes.append(slopes[current - 1] + (2 * current + 1) * values[current])
    return (values, slopes)

def gauss_nodes(degree):
    abscissae = np.cos(np.pi * (np.arange(degree) + 0.75) / (degree + 0.5))
    for unused in range(60):
        values, slopes = legendre_table(degree, abscissae)
        abscissae = abscissae - values[degree] / slopes[degree]
    return np.sort(abscissae)

def operator_tables(degree):
    abscissae = gauss_nodes(degree)
    differ = abscissae[:, None] - abscissae[None, :]
    padded = differ + np.eye(degree)
    weights = 1.0 / np.prod(padded, axis=1)
    derivative = weights[None, :] / weights[:, None] / padded * (1.0 - np.eye(degree))
    derivative = derivative - np.eye(degree) * np.sum(derivative, axis=1)[:, None]
    basis_left = weights / (-1.0 - abscissae)
    basis_left = basis_left / np.sum(basis_left)
    basis_right = weights / (1.0 - abscissae)
    basis_right = basis_right / np.sum(basis_right)
    values, slopes = legendre_table(degree, abscissae)
    right_slope = 0.5 * (slopes[degree - 1] + slopes[degree])
    mirror_values, mirror_slopes = legendre_table(degree, -abscissae)
    left_slope = -0.5 * (mirror_slopes[degree - 1] + mirror_slopes[degree])
    sol_points = degree ** 3
    face_points = degree ** 2
    interp = np.zeros((6 * face_points, sol_points))
    grad_matrix = np.zeros((3 * sol_points, sol_points))
    lift_matrix = np.zeros((3 * sol_points, 6 * face_points))
    div_lift = np.zeros((sol_points, 6 * face_points))
    for sol_index in range(sol_points):
        position = (sol_index // face_points, sol_index // degree % degree, sol_index % degree)
        for direction in range(3):
            others = [position[other_dir] for other_dir in range(3) if other_dir != direction]
            flux_index = others[0] * degree + others[1]
            along_index = position[direction]
            for facing in range(2):
                column = (2 * direction + facing) * face_points + flux_index
                interp[column, sol_index] = (basis_left, basis_right)[facing][along_index]
                correct = (left_slope, right_slope)[facing][along_index]
                lift_matrix[direction * sol_points + sol_index, column] = correct
                div_lift[sol_index, column] = (2 * facing - 1) * correct
            for target in range(degree):
                shifted = list(position)
                shifted[direction] = target
                other_point = (shifted[0] * degree + shifted[1]) * degree + shifted[2]
                grad_matrix[direction * sol_points + sol_index, other_point] = derivative[along_index, target]
    normal_matrix = np.zeros((6 * face_points, 3 * sol_points))
    normals = np.zeros((3, 6))
    for face_id in range(6):
        direction = face_id // 2
        orient = 2 * (face_id % 2) - 1
        rows_here = slice(face_id * face_points, (face_id + 1) * face_points)
        normal_matrix[rows_here, direction * sol_points:(direction + 1) * sol_points] = orient * interp[rows_here]
        normals[direction, face_id] = orient
    div_matrix = np.concatenate([grad_matrix[direction * sol_points:(direction + 1) * sol_points] for direction in range(3)], axis=1)
    tables = (interp, grad_matrix, lift_matrix, normal_matrix, div_matrix, div_lift, normals)
    return tuple((jnp.asarray(source, dtype=jnp.float32) for source in tables))

def exact_dot(matrix, operand):
    return jnp.dot(matrix, operand, precision=lax.Precision.HIGHEST, preferred_element_type=jnp.float32)

def face_layout(matrix, face_points, fields, elements):
    return jnp.transpose(matrix.reshape(6, face_points, fields, elements), (1, 2, 0, 3))

def matrix_layout(faces):
    face_points, fields, sides, elements = faces.shape
    return jnp.transpose(faces, (2, 0, 1, 3)).reshape(sides * face_points, fields * elements)

def split_fields(values):
    return [values[:, field_id] for field_id in range(values.shape[1])]

def primitive(fields):
    density = fields[0]
    velocity = [fields[1 + direction] / density for direction in range(3)]
    kinetic = 0.5 * (fields[1] * velocity[0] + fields[2] * velocity[1] + fields[3] * velocity[2])
    pressure = (heat_ratio - 1.0) * (fields[4] - kinetic)
    return (density, velocity, pressure)

def inviscid_flux(fields, velocity, pressure, direction):
    result = [fields[1 + direction]]
    for component in range(3):
        member = fields[1 + component] * velocity[direction]
        if component == direction:
            member = member + pressure
        result.append(member)
    result.append((fields[4] + pressure) * velocity[direction])
    return result

def viscous_terms(fields, density, velocity, slopes):
    vel_slope = [[(slopes[across][1 + component] - velocity[component] * slopes[across][0]) / density for across in range(3)] for component in range(3)]
    energy_slope = []
    for across in range(3):
        internal = (slopes[across][4] - fields[4] / density * slopes[across][0]) / density
        internal = internal - (velocity[0] * vel_slope[0][across] + velocity[1] * vel_slope[1][across] + velocity[2] * vel_slope[2][across])
        energy_slope.append(internal)
    divergence = vel_slope[0][0] + vel_slope[1][1] + vel_slope[2][2]
    return (vel_slope, energy_slope, divergence)

def viscous_flux(velocity, vel_slope, energy_slope, divergence, direction):
    stress = []
    for component in range(3):
        member = viscosity * (vel_slope[component][direction] + vel_slope[direction][component])
        if component == direction:
            member = member - 2.0 / 3.0 * viscosity * divergence
        stress.append(member)
    work_done = velocity[0] * stress[0] + velocity[1] * stress[1] + velocity[2] * stress[2]
    heat_flux = viscosity * heat_ratio / prandtl * energy_slope[direction]
    return [jnp.zeros_like(divergence)] + stress + [work_done + heat_flux]

def total_flux(fields, slopes):
    density, velocity, pressure = primitive(fields)
    vel_slope, energy_slope, divergence = viscous_terms(fields, density, velocity, slopes)
    result = []
    for direction in range(3):
        inviscid = inviscid_flux(fields, velocity, pressure, direction)
        viscous = viscous_flux(velocity, vel_slope, energy_slope, divergence, direction)
        result.append([inviscid[field_id] - viscous[field_id] for field_id in range(5)])
    return result

def normal_viscous(fields, slopes, weights):
    density, velocity, pressure = primitive(fields)
    vel_slope, energy_slope, divergence = viscous_terms(fields, density, velocity, slopes)
    summed = [0.0] * 5
    for direction in range(3):
        viscous = viscous_flux(velocity, vel_slope, energy_slope, divergence, direction)
        summed = [summed[field_id] + weights[direction] * viscous[field_id] for field_id in range(5)]
    return summed

def common_flux(own_fields, other_fields, own_visc, other_visc, weights):
    rho_left, vel_left, press_left = primitive(own_fields)
    rho_right, vel_right, press_right = primitive(other_fields)
    normal_left = [0.0] * 5
    normal_right = [0.0] * 5
    speed_left = 0.0
    speed_right = 0.0
    for direction in range(3):
        flux_left = inviscid_flux(own_fields, vel_left, press_left, direction)
        flux_right = inviscid_flux(other_fields, vel_right, press_right, direction)
        normal_left = [normal_left[field_id] + weights[direction] * flux_left[field_id] for field_id in range(5)]
        normal_right = [normal_right[field_id] + weights[direction] * flux_right[field_id] for field_id in range(5)]
        speed_left = speed_left + weights[direction] * vel_left[direction]
        speed_right = speed_right + weights[direction] * vel_right[direction]
    wave_left = jnp.abs(speed_left) + jnp.sqrt(heat_ratio * press_left / rho_left)
    wave_right = jnp.abs(speed_right) + jnp.sqrt(heat_ratio * press_right / rho_right)
    wave_speed = jnp.maximum(wave_left, wave_right)
    return [0.5 * (normal_left[field_id] + normal_right[field_id]) - 0.5 * (own_visc[field_id] + other_visc[field_id]) + (0.5 * wave_speed + penalty) * (own_fields[field_id] - other_fields[field_id]) for field_id in range(5)]

def reference(solution, face_link):
    interp, grad_matrix, lift_matrix, normal_matrix, div_matrix, div_lift, normals = operator_tables(ORDER + 1)
    sol_points, fields, all_elems = solution.shape
    face_points = (ORDER + 1) ** 2
    elements = ELEM_DEV
    blocks = all_elems // elements
    weights = [normals[direction].reshape(1, 6, 1) for direction in range(3)]
    block_ids = jnp.arange(blocks, dtype=jnp.int32)

    def block_of(values, block_id):
        return lax.dynamic_slice_in_dim(values, block_id * elements, elements, axis=values.ndim - 1)

    def traces(block_id):
        flat_sol = block_of(solution, block_id).reshape(sol_points, fields * elements)
        return face_layout(exact_dot(interp, flat_sol), face_points, fields, elements)
    own_all = lax.map(traces, block_ids)

    def partner(source, block_id):
        link_block = block_of(face_link, block_id)
        partner_elem = link_block // 6
        picked = source[partner_elem // elements, :, :, link_block % 6, partner_elem % elements]
        return jnp.transpose(picked, (2, 3, 0, 1))

    def gradient(block_id):
        flat_sol = block_of(solution, block_id).reshape(sol_points, fields * elements)
        own_trace = own_all[block_id]
        other_trace = partner(own_all, block_id)
        jump_mat = matrix_layout(0.5 * (other_trace - own_trace))
        grad_field = (exact_dot(grad_matrix, flat_sol) + exact_dot(lift_matrix, jump_mat)).reshape(3, sol_points, fields, elements)
        return (own_trace, other_trace, grad_field)

    def viscous_traces(block_id):
        own_trace, other_trace, grad_field = gradient(block_id)
        spread = jnp.einsum('pq,dqx->dpx', interp, grad_field.reshape(3, sol_points, fields * elements), precision=lax.Precision.HIGHEST)
        traced = jnp.transpose(spread.reshape(3, 6, face_points, fields, elements), (0, 2, 3, 1, 4))
        slopes = [split_fields(traced[direction]) for direction in range(3)]
        return jnp.stack(normal_viscous(split_fields(own_trace), slopes, weights), axis=1)
    visc_all = lax.map(viscous_traces, block_ids)

    def rate_block(block_id):
        own_trace, other_trace, grad_field = gradient(block_id)
        own_visc = split_fields(visc_all[block_id])
        other_visc = [-member for member in split_fields(partner(visc_all, block_id))]
        sol_fields = split_fields(block_of(solution, block_id))
        sol_slopes = [split_fields(grad_field[direction]) for direction in range(3)]
        fluxes = total_flux(sol_fields, sol_slopes)
        flux_mat = jnp.stack([jnp.stack(fluxes[direction], axis=1) for direction in range(3)]).reshape(3 * sol_points, fields * elements)
        own_normal = face_layout(exact_dot(normal_matrix, flux_mat), face_points, fields, elements)
        common = common_flux(split_fields(own_trace), split_fields(other_trace), own_visc, other_visc, weights)
        jump_mat = matrix_layout(jnp.stack(common, axis=1) - own_normal)
        return -(exact_dot(div_matrix, flux_mat) + exact_dot(div_lift, jump_mat)).reshape(sol_points, fields, elements)
    block_rates = lax.map(rate_block, block_ids)
    return jnp.transpose(block_rates, (1, 2, 0, 3)).reshape(sol_points, fields, all_elems)
```

```python
import functools

import jax
import jax.numpy as jnp
import numpy as np
from jax import lax
from jax.experimental import pallas as pl
from jax.experimental.pallas import tpu as pltpu
from jax.sharding import PartitionSpec as P

ORDER = 4

heat_ratio = 1.4
viscosity = 0.08
prandtl = 0.72
penalty = 0.1

LANES = 128
SUBLANES = 8
FIELDS = 5
PAIR = 2
DIRS = 3


def legendre_table(degree, abscissae):
    values = [abscissae * 0.0 + 1.0, abscissae.copy()]
    slopes = [abscissae * 0.0, abscissae * 0.0 + 1.0]
    for current in range(1, degree):
        values.append(
            ((2 * current + 1) * abscissae * values[current] - current * values[current - 1])
            / (current + 1)
        )
        slopes.append(slopes[current - 1] + (2 * current + 1) * values[current])
    return (values, slopes)


def gauss_nodes(degree):
    abscissae = np.cos(np.pi * (np.arange(degree) + 0.75) / (degree + 0.5))
    for unused in range(60):
        values, slopes = legendre_table(degree, abscissae)
        abscissae = abscissae - values[degree] / slopes[degree]
    return np.sort(abscissae)


def operator_tables(degree):
    abscissae = gauss_nodes(degree)
    differ = abscissae[:, None] - abscissae[None, :]
    padded = differ + np.eye(degree)
    weights = 1.0 / np.prod(padded, axis=1)
    derivative = weights[None, :] / weights[:, None] / padded * (1.0 - np.eye(degree))
    derivative = derivative - np.eye(degree) * np.sum(derivative, axis=1)[:, None]
    basis_left = weights / (-1.0 - abscissae)
    basis_left = basis_left / np.sum(basis_left)
    basis_right = weights / (1.0 - abscissae)
    basis_right = basis_right / np.sum(basis_right)
    values, slopes = legendre_table(degree, abscissae)
    right_slope = 0.5 * (slopes[degree - 1] + slopes[degree])
    mirror_values, mirror_slopes = legendre_table(degree, -abscissae)
    left_slope = -0.5 * (mirror_slopes[degree - 1] + mirror_slopes[degree])
    sol_points = degree**3
    face_points = degree**2
    interp = np.zeros((6 * face_points, sol_points))
    grad_matrix = np.zeros((3 * sol_points, sol_points))
    lift_matrix = np.zeros((3 * sol_points, 6 * face_points))
    div_lift = np.zeros((sol_points, 6 * face_points))
    for sol_index in range(sol_points):
        position = (sol_index // face_points, sol_index // degree % degree, sol_index % degree)
        for direction in range(3):
            others = [position[other_dir] for other_dir in range(3) if other_dir != direction]
            flux_index = others[0] * degree + others[1]
            along_index = position[direction]
            for facing in range(2):
                column = (2 * direction + facing) * face_points + flux_index
                interp[column, sol_index] = (basis_left, basis_right)[facing][along_index]
                correct = (left_slope, right_slope)[facing][along_index]
                lift_matrix[direction * sol_points + sol_index, column] = correct
                div_lift[sol_index, column] = (2 * facing - 1) * correct
            for target in range(degree):
                shifted = list(position)
                shifted[direction] = target
                other_point = (shifted[0] * degree + shifted[1]) * degree + shifted[2]
                grad_matrix[direction * sol_points + sol_index, other_point] = derivative[
                    along_index, target
                ]
    return interp, grad_matrix, lift_matrix, div_lift


def face_col(face, face_points):
    return face // 3 * LANES + face % 3 * face_points


def split_table(table):
    full = table.astype(np.float32)
    high = full.astype(jnp.bfloat16)
    low = (full - high.astype(np.float32)).astype(jnp.bfloat16)
    return np.stack([high, low])


@functools.lru_cache(None)
def padded_tables(degree):
    interp, grad_matrix, lift_matrix, div_lift = operator_tables(degree)
    sol_points = degree**3
    face_points = degree**2
    width = 2 * LANES
    cols = np.array(
        [face_col(face, face_points) + q for face in range(6) for q in range(face_points)]
    )
    spread = np.zeros((LANES, width))
    spread[:sol_points, cols] = interp.T
    grad = np.zeros((LANES, DIRS * LANES))
    lift = np.zeros((width, DIRS * LANES))
    div = np.zeros((DIRS * LANES, LANES))
    normal = np.zeros((DIRS * LANES, width))
    normals = np.zeros((SUBLANES, width))
    for d in range(DIRS):
        part = slice(d * sol_points, (d + 1) * sol_points)
        here = slice(d * LANES, d * LANES + sol_points)
        grad[:sol_points, here] = grad_matrix[part].T
        lift[cols, here] = lift_matrix[part].T
        div[here, :sol_points] = grad_matrix[part].T
        for side in range(2):
            face = 2 * d + side
            start = face_col(face, face_points)
            rows = slice(face * face_points, (face + 1) * face_points)
            normal[here, start : start + face_points] = (2 * side - 1) * interp[rows].T
            normals[d, start : start + face_points] = 2 * side - 1
    drop = np.zeros((width, LANES))
    drop[cols, :sol_points] = div_lift.T
    normals[DIRS] = 1.0
    normals[DIRS, cols] = 0.0
    tables = [split_table(t) for t in (spread, grad, lift, normal, div, drop)]
    return tables + [normals.astype(np.float32)]


def dot16(left, right):
    return jnp.dot(left, right, preferred_element_type=jnp.float32)


def halves(values):
    high = values.astype(jnp.bfloat16)
    low = (values - high.astype(jnp.float32)).astype(jnp.bfloat16)
    return high, low


def table_dot(values, table):
    high, low = halves(values)
    return dot16(high, table[0]) + (dot16(high, table[1]) + dot16(low, table[0]))


def pick_rows(chooser, values):
    high = values.astype(jnp.bfloat16)
    rest = values - high.astype(jnp.float32)
    middle = rest.astype(jnp.bfloat16)
    low = (rest - middle.astype(jnp.float32)).astype(jnp.bfloat16)
    return dot16(chooser, high) + (dot16(chooser, middle) + dot16(chooser, low))


def floor_by(values, divisor):
    scaled = (values.astype(jnp.float32) + 0.5) * (1.0 / divisor)
    return jnp.floor(scaled).astype(jnp.int32)


def wrap(values, size):
    return jnp.where(values < 0, values + size, values)


def link_row(link_ref, row_ref, elements):
    row_ref[...] = jnp.full_like(row_ref, -1)
    for face in range(6):
        row_ref[0:1, face * elements : (face + 1) * elements] = link_ref[face : face + 1, :]
    return row_ref[0:1, :]


def partner_place(link, elements, dom_count, sub_count):
    my_dom = lax.axis_index("dom")
    my_sub = lax.axis_index("sub")
    my_chip = my_dom // PAIR
    my_core = my_dom % PAIR
    partner = floor_by(link, 6)
    key = (link - 6 * partner) * elements
    device = floor_by(partner, elements)
    key = key + partner - device * elements
    dom = floor_by(device, sub_count)
    sub = device - dom * sub_count
    chip = floor_by(dom, PAIR)
    core = dom - PAIR * chip
    step = wrap(chip - my_chip, dom_count // PAIR)
    side = jnp.where(step == 0, 0, jnp.where(step == 1, 1, 2))
    flip = jnp.where(core == my_core, 0, 1)
    ahead = wrap(sub - my_sub, sub_count)
    back = wrap(my_sub - sub, sub_count)
    return device, key, side, flip, ahead, back


def to_faces(source, face_ref, elements, face_points, fields):
    for face in range(6):
        start = face_col(face, face_points)
        for slot, field in enumerate(fields):
            face_ref[
                face * elements : (face + 1) * elements,
                field * face_points : (field + 1) * face_points,
            ] = source[slot * elements : (slot + 1) * elements, start : start + face_points]


def from_faces(faces, target_ref, elements, face_points, fields):
    for face in range(6):
        start = face_col(face, face_points)
        for slot, field in enumerate(fields):
            target_ref[
                slot * elements : (slot + 1) * elements, start : start + face_points
            ] = faces[
                face * elements : (face + 1) * elements,
                field * face_points : (field + 1) * face_points,
            ]


def pack_kernel(
    sizes, sol_hbm, link_hbm, spread_hbm, normals_hbm, *refs
):
    mates = PAIR * sizes[4]
    msg_refs = refs[:mates]
    (
        trace_ref, face_ref, choose_ref, pad_ref,
        row_ref, sol_ref, link_ref, spread_ref, normals_ref, sems,
    ) = refs[mates:]
    elements, sol_points, face_points, dom_count, sub_count, rows = sizes
    groups = DIRS * PAIR * sub_count
    loads = [
        pltpu.make_async_copy(source, target, sems.at[i])
        for i, (source, target) in enumerate(
            [
                (link_hbm, link_ref),
                (sol_hbm, sol_ref),
                (spread_hbm, spread_ref),
                (normals_hbm, normals_ref),
            ]
        )
    ]
    for load in loads:
        load.start()
    lanes = row_ref.shape[1]
    order = (
        lax.broadcasted_iota(jnp.int32, (lanes, lanes), 0)
        < lax.broadcasted_iota(jnp.int32, (lanes, lanes), 1)
    ).astype(jnp.float32).astype(jnp.bfloat16)
    face_ref[...] = jnp.zeros_like(face_ref)
    pad_ref[...] = jnp.ones_like(pad_ref)
    loads[0].wait()
    link = link_row(link_ref, row_ref, elements)
    device, key, side, flip, ahead, back = partner_place(link, elements, dom_count, sub_count)
    group = (flip * sub_count + ahead) * DIRS + side
    group = jnp.where(link < 0, -1, group)
    group_rows = -(-groups // 16) * 16
    width = group.shape[1]
    row_ids = lax.broadcasted_iota(jnp.int32, (group_rows, width), 0)
    member = (row_ids == group).astype(jnp.float32)
    before = dot16(member.astype(jnp.bfloat16), order)
    rank = jnp.sum(member * before, axis=0, keepdims=True).astype(jnp.int32)
    slot = jnp.where(group <= 0, -1, group * rows + rank)
    slot_ids = lax.broadcasted_iota(jnp.int32, (groups * rows, width), 0)
    chooser = (slot_ids == slot).astype(jnp.float32).astype(jnp.bfloat16)
    choose_ref[...] = chooser
    for load in loads[1:]:
        load.wait()
    pad_ref[:, :sol_points] = sol_ref[...]
    trace = table_dot(pad_ref[...], spread_ref)
    trace_ref[...] = trace
    still = normals_ref[DIRS : DIRS + 1, :]
    for k in (0, FIELDS - 1):
        part = slice(k * elements, (k + 1) * elements)
        trace_ref[part] = trace_ref[part] + still
    to_faces(trace, face_ref, elements, face_points, range(FIELDS))
    store_message(pick_rows(chooser, face_ref[...]), msg_refs)


def route_kernel(
    sizes, pad_ref, link_ref, face_ref, grad_ref,
    remote_ref, local_ref, near_ref, slope_ref, row_ref,
):
    elements, sol_points, face_points, dom_count, sub_count, rows = sizes
    faces = 6 * elements
    link = link_row(link_ref, row_ref, elements)
    device, key, side, flip, ahead, back = partner_place(link, elements, dom_count, sub_count)
    mate = flip * sub_count + back
    is_local = (side == 0) & (mate == 0)
    side = jnp.where(side == 0, 0, 3 - side)
    base = jnp.where(is_local, -faces, (side * PAIR * sub_count + mate) * rows)
    lowest = jnp.where(link < 0, -4 * faces, device * faces)
    total = jnp.where(link < 0, -2 * faces, lowest + key)
    width = link.shape[1]
    stack = jnp.concatenate(
        [
            total.astype(jnp.float32),
            lowest.astype(jnp.float32),
            base.astype(jnp.float32),
            jnp.where(is_local, key, -1).astype(jnp.float32),
            jnp.zeros((SUBLANES - 4, width), jnp.float32),
        ],
        axis=0,
    )
    flipped = jnp.transpose(stack)[:faces]
    col = [flipped[:, i : i + 1] for i in range(4)]
    total_row = total.astype(jnp.float32)
    hits = (total_row < col[0]) & (total_row >= col[1])
    rank = jnp.sum(hits.astype(jnp.float32), axis=1, keepdims=True)
    slot = (col[2] + rank).astype(jnp.int32)
    slots = remote_ref.shape[1]
    lane_ids = lax.broadcasted_iota(jnp.int32, (faces, slots), 1)
    remote_ref[...] = (lane_ids == slot).astype(jnp.float32).astype(jnp.bfloat16)
    face_ids = lax.broadcasted_iota(jnp.int32, (faces, width), 1)
    local = (face_ids == col[3].astype(jnp.int32)).astype(jnp.float32).astype(jnp.bfloat16)
    local_ref[...] = local
    near_ref[...] = pick_rows(local, face_ref[...])
    slope_ref[...] = table_dot(pad_ref[...], grad_ref)


def primitive(fields):
    inverse = 1.0 / fields[0]
    velocity = [fields[1 + d] * inverse for d in range(DIRS)]
    kinetic = 0.5 * (fields[1] * velocity[0] + fields[2] * velocity[1] + fields[3] * velocity[2])
    pressure = (heat_ratio - 1.0) * (fields[4] - kinetic)
    return inverse, velocity, pressure


def viscous_terms(fields, inverse, velocity, slopes):
    vel_slope = [
        [(slopes[a][1 + b] - velocity[b] * slopes[a][0]) * inverse for a in range(DIRS)]
        for b in range(DIRS)
    ]
    specific = fields[4] * inverse
    energy_slope = [
        (slopes[a][4] - specific * slopes[a][0]) * inverse
        - (
            velocity[0] * vel_slope[0][a]
            + velocity[1] * vel_slope[1][a]
            + velocity[2] * vel_slope[2][a]
        )
        for a in range(DIRS)
    ]
    divergence = vel_slope[0][0] + vel_slope[1][1] + vel_slope[2][2]
    return vel_slope, energy_slope, divergence


def viscous_flux(velocity, vel_slope, energy_slope, divergence, a):
    stress = []
    for b in range(DIRS):
        member = viscosity * (vel_slope[b][a] + vel_slope[a][b])
        if a == b:
            member = member - 2.0 / 3.0 * viscosity * divergence
        stress.append(member)
    work = velocity[0] * stress[0] + velocity[1] * stress[1] + velocity[2] * stress[2]
    return stress + [work + viscosity * heat_ratio / prandtl * energy_slope[a]]


def field_rows(values, elements, count):
    return [values[k * elements : (k + 1) * elements] for k in range(count)]


def gather_message(parts, scratch_ref, rows, mates):
    mate_refs, first_far, second_far = parts
    scratch_ref[...] = jnp.zeros_like(scratch_ref)
    for index, ref in enumerate(mate_refs):
        scratch_ref[(index + 1) * rows : (index + 2) * rows] = ref[:rows]
    scratch_ref[mates * rows : 2 * mates * rows] = first_far[...]
    scratch_ref[2 * mates * rows : 3 * mates * rows] = second_far[...]
    return scratch_ref[...]


def store_message(message, msg_refs):
    height = message.shape[0] // len(msg_refs)
    for mate, ref in enumerate(msg_refs):
        ref[...] = message[mate * height : (mate + 1) * height]


def gradient_kernel(sizes, mates, *refs):
    elements, sol_points, face_points, dom_count, sub_count, rows = sizes
    mate_refs = refs[: mates - 1]
    (
        first_ref, second_ref, remote_ref, near_ref, slope_ref, trace_ref, choose_ref,
        lift_ref, spread_ref, normals_ref,
    ) = refs[mates - 1 : mates + 9]
    msg_refs = refs[mates + 9 : 2 * mates + 9]
    other_ref, grad_ref, visc_ref, vface_ref, arrived_ref = refs[2 * mates + 9 :]
    arrived = gather_message((mate_refs, first_ref, second_ref), arrived_ref, rows, mates)
    faces = near_ref[...] + pick_rows(remote_ref[...], arrived)
    for k in range(FIELDS):
        part = slice(k * elements, (k + 1) * elements)
        fill = 1.0 if k in (0, FIELDS - 1) else 0.0
        other_ref[part] = jnp.full((elements, other_ref.shape[1]), fill, jnp.float32)
    from_faces(faces, other_ref, elements, face_points, range(FIELDS))
    trace = trace_ref[...]
    jump = 0.5 * (other_ref[...] - trace)
    grad = slope_ref[...] + table_dot(jump, lift_ref)
    grad_ref[...] = grad
    slopes = []
    for a in range(DIRS):
        traced = table_dot(grad[:, a * LANES : (a + 1) * LANES], spread_ref)
        slopes.append(field_rows(traced, elements, FIELDS))
    fields = field_rows(trace, elements, FIELDS)
    inverse, velocity, pressure = primitive(fields)
    vel_slope, energy_slope, divergence = viscous_terms(fields, inverse, velocity, slopes)
    weights = [normals_ref[a : a + 1, :] for a in range(DIRS)]
    summed = [0.0] * 4
    for a in range(DIRS):
        viscous = viscous_flux(velocity, vel_slope, energy_slope, divergence, a)
        summed = [summed[i] + weights[a] * viscous[i] for i in range(4)]
    vface_ref[...] = jnp.zeros_like(vface_ref)
    for i in range(4):
        visc_ref[i * elements : (i + 1) * elements] = summed[i]
    to_faces(visc_ref, vface_ref, elements, face_points, range(1, FIELDS))
    store_message(pick_rows(choose_ref[...], vface_ref[...]), msg_refs)


def volume_kernel(
    sizes, pad_ref, grad_ref, trace_ref, other_ref, visc_ref, vface_ref, local_ref,
    normal_ref, div_ref, drop_ref, normals_ref,
    partial_ref, near_ref, flux_ref, jump_ref,
):
    elements, sol_points, face_points, dom_count, sub_count, rows = sizes
    near_ref[...] = pick_rows(local_ref[...], vface_ref[...])
    fields = field_rows(pad_ref[...], elements, FIELDS)
    grad = grad_ref[...]
    slopes = [
        field_rows(grad[:, a * LANES : (a + 1) * LANES], elements, FIELDS) for a in range(DIRS)
    ]
    inverse, velocity, pressure = primitive(fields)
    vel_slope, energy_slope, divergence = viscous_terms(fields, inverse, velocity, slopes)
    for a in range(DIRS):
        viscous = viscous_flux(velocity, vel_slope, energy_slope, divergence, a)
        flux = [fields[1 + a]]
        for b in range(DIRS):
            member = fields[1 + b] * velocity[a]
            if a == b:
                member = member + pressure
            flux.append(member - viscous[b])
        flux.append((fields[4] + pressure) * velocity[a] - viscous[3])
        for k in range(FIELDS):
            flux_ref[k * elements : (k + 1) * elements, a * LANES : (a + 1) * LANES] = flux[k]
    flux = flux_ref[...]
    weights = [normals_ref[a : a + 1, :] for a in range(DIRS)]
    own = field_rows(trace_ref[...], elements, FIELDS)
    other = field_rows(other_ref[...], elements, FIELDS)
    inv_l, vel_l, press_l = primitive(own)
    inv_r, vel_r, press_r = primitive(other)
    speed_l = weights[0] * vel_l[0] + weights[1] * vel_l[1] + weights[2] * vel_l[2]
    speed_r = weights[0] * vel_r[0] + weights[1] * vel_r[1] + weights[2] * vel_r[2]
    wave_l = jnp.abs(speed_l) + jnp.sqrt(heat_ratio * press_l * inv_l)
    wave_r = jnp.abs(speed_r) + jnp.sqrt(heat_ratio * press_r * inv_r)
    upwind = 0.5 * jnp.maximum(wave_l, wave_r) + penalty
    press = press_l + press_r
    for k in range(FIELDS):
        central = own[k] * speed_l + other[k] * speed_r
        if k == 4:
            central = central + press_l * speed_l + press_r * speed_r
        elif k > 0:
            central = central + weights[k - 1] * press
        member = 0.5 * central + upwind * (own[k] - other[k])
        if k > 0:
            member = member - 0.5 * visc_ref[(k - 1) * elements : k * elements]
        jump_ref[k * elements : (k + 1) * elements] = member
    jump = jump_ref[...] - table_dot(flux, normal_ref)
    partial_ref[...] = table_dot(flux, div_ref) + table_dot(jump, drop_ref)


def final_kernel(sizes, mates, *refs):
    elements, sol_points, face_points, dom_count, sub_count, rows = sizes
    mate_refs = refs[: mates - 1]
    first_ref, second_ref, remote_ref, near_ref, partial_ref, drop_ref = refs[mates - 1 : mates + 5]
    rate_ref, arrived_ref, visc_ref = refs[mates + 5 :]
    arrived = gather_message((mate_refs, first_ref, second_ref), arrived_ref, rows, mates)
    faces = near_ref[...] + pick_rows(remote_ref[...], arrived)
    visc_ref[...] = jnp.zeros_like(visc_ref)
    from_faces(faces, visc_ref, elements, face_points, range(1, FIELDS))
    partial = partial_ref[...]
    lifted = table_dot(0.5 * visc_ref[...], drop_ref)
    rate_ref[:elements] = -partial[:elements, :sol_points]
    rate_ref[elements:] = -(partial[elements:] + lifted)[:, :sol_points]


def run_kernel(body, outs, scratch, *operands, space=pltpu.VMEM, limit=16 << 20):
    vmem = pl.BlockSpec(memory_space=pltpu.VMEM)
    if space == pltpu.HBM:
        operands = [pltpu.with_memory_space_constraint(x, pltpu.HBM) for x in operands]
    return pl.pallas_call(
        body,
        out_shape=outs,
        in_specs=[pl.BlockSpec(memory_space=space)] * len(operands),
        out_specs=jax.tree.map(lambda _: vmem, outs),
        scratch_shapes=scratch,
        compiler_params=pltpu.CompilerParams(vmem_limit_bytes=limit),
        cost_estimate=pl.CostEstimate(flops=2 << 30, bytes_accessed=1 << 20, transcendentals=0),
    )(*operands)


def shape_of(shape, dtype=jnp.float32):
    return jax.ShapeDtypeStruct(shape, dtype)


def exchange(blocks, sub_count, dom_count, rows):
    mates = PAIR * sub_count
    arrived = [blocks[0]]
    for mate in range(1, mates):
        flip, shift = divmod(mate, sub_count)
        route = [
            (d * sub_count + s, (d ^ flip) * sub_count + (s + shift) % sub_count)
            for d in range(dom_count)
            for s in range(sub_count)
        ]
        arrived.append(lax.ppermute(blocks[mate], ("dom", "sub"), route))
    far = []
    for side in (1, 2):
        packed = jnp.concatenate([block[side * rows : (side + 1) * rows] for block in arrived])
        hop = PAIR if side == 1 else -PAIR
        route = [(d, (d + hop) % dom_count) for d in range(dom_count)]
        far.append(lax.ppermute(packed, "dom", route))
    return arrived[1:] + far


def shards(solution, face_link):
    spread, grad, lift, normal, div, drop, normals = padded_tables(ORDER + 1)
    sol_points, fields, elements = solution.shape
    face_points = (ORDER + 1) ** 2
    sub_count = lax.axis_size("sub")
    dom_count = lax.axis_size("dom")
    capacity = max(3, elements * 3 // 16)
    rows = -(-capacity // SUBLANES) * SUBLANES
    mates = PAIR * sub_count
    slots = DIRS * mates * rows
    slot_lanes = -(-slots // LANES) * LANES
    faces = 6 * elements
    face_lanes = -(-faces // LANES) * LANES
    sizes = (elements, sol_points, face_points, dom_count, sub_count, rows)
    row_scratch = pltpu.VMEM((1, face_lanes), jnp.int32)
    tall = fields * elements
    width = 2 * LANES
    sol = jnp.transpose(solution, (1, 2, 0)).reshape(tall, sol_points)

    blocks = [shape_of((slots // mates, LANES))] * mates
    *msg, trace, face, choose, padded = run_kernel(
        functools.partial(pack_kernel, sizes),
        (
            *blocks,
            shape_of((tall, width)),
            shape_of((face_lanes, LANES)),
            shape_of((slots, face_lanes), jnp.bfloat16),
            shape_of((tall, LANES)),
        ),
        [
            row_scratch,
            pltpu.VMEM(sol.shape, jnp.float32),
            pltpu.VMEM(face_link.shape, jnp.int32),
            pltpu.VMEM(spread.shape, jnp.bfloat16),
            pltpu.VMEM(normals.shape, jnp.float32),
            pltpu.SemaphoreType.DMA((4,)),
        ],
        sol, face_link, spread, normals,
        space=pltpu.HBM,
    )
    pieces = exchange(msg, sub_count, dom_count, rows)
    remote, local, near, slope = run_kernel(
        functools.partial(route_kernel, sizes),
        (
            shape_of((faces, slot_lanes), jnp.bfloat16),
            shape_of((faces, face_lanes), jnp.bfloat16),
            shape_of((faces, LANES)),
            shape_of((tall, DIRS * LANES)),
        ),
        [row_scratch],
        padded, face_link, face, grad,
    )
    *msg, other, slopes, visc, vface = run_kernel(
        functools.partial(gradient_kernel, sizes, mates),
        (
            *blocks,
            shape_of((tall, width)),
            shape_of((tall, DIRS * LANES)),
            shape_of((tall - elements, width)),
            shape_of((face_lanes, LANES)),
        ),
        [pltpu.VMEM((slot_lanes, LANES), jnp.float32)],
        *pieces, remote, near, slope, trace, choose, lift, spread, normals,
    )
    pieces = exchange(msg, sub_count, dom_count, rows)
    partial, near = run_kernel(
        functools.partial(volume_kernel, sizes),
        (shape_of((tall, LANES)), shape_of((faces, LANES))),
        [
            pltpu.VMEM((tall, DIRS * LANES), jnp.float32),
            pltpu.VMEM((tall, width), jnp.float32),
        ],
        padded, slopes, trace, other, visc, vface, local, normal, div, drop, normals,
    )
    rate = run_kernel(
        functools.partial(final_kernel, sizes, mates),
        shape_of((tall, sol_points)),
        [
            pltpu.VMEM((slot_lanes, LANES), jnp.float32),
            pltpu.VMEM((tall - elements, width), jnp.float32),
        ],
        *pieces, remote, near, partial, drop,
    )
    return jnp.transpose(rate.reshape(fields, elements, sol_points), (2, 0, 1))


def solution(mesh):
    in_specs = (P(None, None, ("dom", "sub")), P(None, ("dom", "sub")))
    out_specs = P(None, None, ("dom", "sub"))
    return jax.shard_map(shards, mesh=mesh, in_specs=in_specs, out_specs=out_specs, check_vma=False)
```

```python
import functools

import jax
import jax.numpy as jnp
import numpy as np
from jax import lax
from jax.experimental import pallas as pl
from jax.experimental.pallas import tpu as pltpu
from jax.sharding import PartitionSpec as P

ORDER = 4

heat_ratio = 1.4
viscosity = 0.08
prandtl = 0.72
penalty = 0.1

LANES = 128
SUBLANES = 8
FIELDS = 5
PAIR = 2
DIRS = 3


def legendre_table(degree, abscissae):
    values = [abscissae * 0.0 + 1.0, abscissae.copy()]
    slopes = [abscissae * 0.0, abscissae * 0.0 + 1.0]
    for current in range(1, degree):
        values.append(
            ((2 * current + 1) * abscissae * values[current] - current * values[current - 1])
            / (current + 1)
        )
        slopes.append(slopes[current - 1] + (2 * current + 1) * values[current])
    return (values, slopes)


def gauss_nodes(degree):
    abscissae = np.cos(np.pi * (np.arange(degree) + 0.75) / (degree + 0.5))
    for unused in range(60):
        values, slopes = legendre_table(degree, abscissae)
        abscissae = abscissae - values[degree] / slopes[degree]
    return np.sort(abscissae)


def operator_tables(degree):
    abscissae = gauss_nodes(degree)
    differ = abscissae[:, None] - abscissae[None, :]
    padded = differ + np.eye(degree)
    weights = 1.0 / np.prod(padded, axis=1)
    derivative = weights[None, :] / weights[:, None] / padded * (1.0 - np.eye(degree))
    derivative = derivative - np.eye(degree) * np.sum(derivative, axis=1)[:, None]
    basis_left = weights / (-1.0 - abscissae)
    basis_left = basis_left / np.sum(basis_left)
    basis_right = weights / (1.0 - abscissae)
    basis_right = basis_right / np.sum(basis_right)
    values, slopes = legendre_table(degree, abscissae)
    right_slope = 0.5 * (slopes[degree - 1] + slopes[degree])
    mirror_values, mirror_slopes = legendre_table(degree, -abscissae)
    left_slope = -0.5 * (mirror_slopes[degree - 1] + mirror_slopes[degree])
    sol_points = degree**3
    face_points = degree**2
    interp = np.zeros((6 * face_points, sol_points))
    grad_matrix = np.zeros((3 * sol_points, sol_points))
    lift_matrix = np.zeros((3 * sol_points, 6 * face_points))
    div_lift = np.zeros((sol_points, 6 * face_points))
    for sol_index in range(sol_points):
        position = (sol_index // face_points, sol_index // degree % degree, sol_index % degree)
        for direction in range(3):
            others = [position[other_dir] for other_dir in range(3) if other_dir != direction]
            flux_index = others[0] * degree + others[1]
            along_index = position[direction]
            for facing in range(2):
                column = (2 * direction + facing) * face_points + flux_index
                interp[column, sol_index] = (basis_left, basis_right)[facing][along_index]
                correct = (left_slope, right_slope)[facing][along_index]
                lift_matrix[direction * sol_points + sol_index, column] = correct
                div_lift[sol_index, column] = (2 * facing - 1) * correct
            for target in range(degree):
                shifted = list(position)
                shifted[direction] = target
                other_point = (shifted[0] * degree + shifted[1]) * degree + shifted[2]
                grad_matrix[direction * sol_points + sol_index, other_point] = derivative[
                    along_index, target
                ]
    return interp, grad_matrix, lift_matrix, div_lift


def face_col(face, face_points):
    return face // 3 * LANES + face % 3 * face_points


def split_table(table):
    full = table.astype(np.float32)
    high = full.astype(jnp.bfloat16)
    low = (full - high.astype(np.float32)).astype(jnp.bfloat16)
    return np.concatenate([high, low])


@functools.lru_cache(None)
def padded_tables(degree):
    interp, grad_matrix, lift_matrix, div_lift = operator_tables(degree)
    sol_points = degree**3
    face_points = degree**2
    width = 2 * LANES
    cols = np.array(
        [face_col(face, face_points) + q for face in range(6) for q in range(face_points)]
    )
    spread = np.zeros((LANES, width))
    spread[:sol_points, cols] = interp.T
    grad = np.zeros((LANES, DIRS * LANES))
    lift = np.zeros((width, DIRS * LANES))
    div = np.zeros((DIRS * LANES, LANES))
    normal = np.zeros((DIRS * LANES, width))
    for d in range(DIRS):
        part = slice(d * sol_points, (d + 1) * sol_points)
        here = slice(d * LANES, d * LANES + sol_points)
        grad[:sol_points, here] = grad_matrix[part].T
        lift[cols, here] = lift_matrix[part].T
        div[here, :sol_points] = grad_matrix[part].T
        for side in range(2):
            face = 2 * d + side
            start = face_col(face, face_points)
            rows = slice(face * face_points, (face + 1) * face_points)
            normal[here, start : start + face_points] = (2 * side - 1) * interp[rows].T
    drop = np.zeros((width, LANES))
    drop[cols, :sol_points] = div_lift.T

    def traced(table):
        parts = [table[:, d * LANES : (d + 1) * LANES] @ spread for d in range(DIRS)]
        return np.concatenate(parts, axis=1)

    tables = (spread, grad, lift, normal, div, drop, traced(grad), traced(lift))
    return [split_table(t) for t in tables]


def dot16(left, right):
    return jnp.dot(left, right, preferred_element_type=jnp.float32)


def halves(values):
    high = values.astype(jnp.bfloat16)
    low = (values - high.astype(jnp.float32)).astype(jnp.bfloat16)
    return high, low


def table_dot(values, table):
    high, low = halves(values)
    both = table[...]
    stacked = jnp.concatenate([both, both[: values.shape[1]]], axis=0)
    return dot16(jnp.concatenate([high, high, low], axis=1), stacked)


def pick_rows(chooser, values):
    high = values.astype(jnp.bfloat16)
    rest = values - high.astype(jnp.float32)
    middle = rest.astype(jnp.bfloat16)
    low = (rest - middle.astype(jnp.float32)).astype(jnp.bfloat16)
    return dot16(
        jnp.concatenate([chooser] * 3, axis=1), jnp.concatenate([high, middle, low], axis=0)
    )


def pick_short(chooser, values):
    return dot16(
        jnp.concatenate([chooser] * 2, axis=1), jnp.concatenate(halves(values), axis=0)
    )


def centred(values, sol_points):
    middle = sol_points // 2
    return values - values[:, middle : middle + 1]


def lane_ids(shape):
    return lax.broadcasted_iota(jnp.int32, shape, 1)


def side_sign(tile, shape, face_points):
    lanes = lane_ids(shape)
    outer = 2.0 * (tile % 2) - 1.0
    middle = (lanes >= face_points) & (lanes < 2 * face_points)
    sign = jnp.where(middle, -outer, outer)
    return jnp.where(lanes < 3 * face_points, sign, 0.0)


def first_direction(tile, shape, face_points):
    return lane_ids(shape) < (2 - tile) * face_points


def floor_by(values, divisor):
    scaled = (values.astype(jnp.float32) + 0.5) * (1.0 / divisor)
    return jnp.floor(scaled).astype(jnp.int32)


def wrap(values, size):
    return jnp.where(values < 0, values + size, values)


def link_row(link_ref, row_ref, elements):
    row_ref[...] = jnp.full_like(row_ref, -1)
    for face in range(6):
        row_ref[0:1, face * elements : (face + 1) * elements] = link_ref[face : face + 1, :]
    return row_ref[0:1, :]


def partner_place(link, elements, dom_count, sub_count):
    my_dom = lax.axis_index("dom")
    my_sub = lax.axis_index("sub")
    my_chip = my_dom // PAIR
    my_core = my_dom % PAIR
    partner = floor_by(link, 6)
    key = (link - 6 * partner) * elements
    device = floor_by(partner, elements)
    key = key + partner - device * elements
    dom = floor_by(device, sub_count)
    sub = device - dom * sub_count
    chip = floor_by(dom, PAIR)
    core = dom - PAIR * chip
    step = wrap(chip - my_chip, dom_count // PAIR)
    side = jnp.where(step == 0, 0, jnp.where(step == 1, 1, 2))
    flip = jnp.where(core == my_core, 0, 1)
    ahead = wrap(sub - my_sub, sub_count)
    back = wrap(my_sub - sub, sub_count)
    return device, key, side, flip, ahead, back


def swap_blocks(take, sources, targets, face_points, base):
    shape = base[0].shape
    lanes = lane_ids(shape)
    inside = [
        (lanes >= b * face_points) & (lanes < (b + 1) * face_points)
        for b in range(max(max(sources), max(targets)) + 1)
    ]
    result = list(base)
    for distance in range(min(sources) - max(targets), max(sources) - min(targets) + 1):
        pairs = [(t + distance, t) for t in targets if t + distance in sources]
        moved = take(pairs[0][0])
        for source, target in pairs[1:]:
            moved = jnp.where(inside[target], take(source), moved)
        shift = distance * face_points % LANES
        moved = pltpu.roll(moved, shift, 1) if shift else moved
        for source, target in pairs:
            index = targets.index(target)
            result[index] = jnp.where(inside[source], moved, result[index])
    return result


def to_faces(tile_of, elements, face_points, fields):
    blank = jnp.zeros((elements, LANES), jnp.float32)
    blocks = []
    for tile in range(2):
        take = lambda field: tile_of(fields.index(field), tile)
        blocks += swap_blocks(take, fields, [0, 1, 2], face_points, [blank] * 3)
    return blocks


def from_faces(faces, fields, tile, base, elements, face_points):
    def take(place):
        face = 3 * tile + place
        return faces[face * elements : (face + 1) * elements]

    return swap_blocks(take, [0, 1, 2], fields, face_points, base)


def tile_reader(ref, elements):
    def read(slot, tile):
        return ref[slot * elements : (slot + 1) * elements, tile * LANES : (tile + 1) * LANES]

    return read


def pack_kernel(
    sizes, sol_hbm, link_hbm, spread_hbm, *refs
):
    mates = PAIR * sizes[4]
    msg_refs = refs[:mates]
    (
        trace_ref, face_ref, choose_ref, pad_ref,
        row_ref, sol_ref, link_ref, spread_ref, sems,
    ) = refs[mates:]
    elements, sol_points, face_points, dom_count, sub_count, rows = sizes
    groups = DIRS * PAIR * sub_count
    loads = [
        pltpu.make_async_copy(source, target, sems.at[i])
        for i, (source, target) in enumerate(
            [
                (link_hbm, link_ref),
                (sol_hbm, sol_ref),
                (spread_hbm, spread_ref),
            ]
        )
    ]
    for load in loads:
        load.start()
    lanes = row_ref.shape[1]
    order = (
        lax.broadcasted_iota(jnp.int32, (lanes, lanes), 0)
        < lax.broadcasted_iota(jnp.int32, (lanes, lanes), 1)
    ).astype(jnp.float32).astype(jnp.bfloat16)
    face_ref[6 * elements :] = jnp.zeros_like(face_ref[6 * elements :])
    pad_ref[...] = jnp.zeros_like(pad_ref)
    loads[0].wait()
    link = link_row(link_ref, row_ref, elements)
    device, key, side, flip, ahead, back = partner_place(link, elements, dom_count, sub_count)
    group = (flip * sub_count + ahead) * DIRS + side
    group = jnp.where(link < 0, -1, group)
    group_rows = -(-groups // 16) * 16
    width = group.shape[1]
    row_ids = lax.broadcasted_iota(jnp.int32, (group_rows, width), 0)
    member = (row_ids == group).astype(jnp.float32)
    before = dot16(member.astype(jnp.bfloat16), order)
    rank = jnp.sum(member * before, axis=0, keepdims=True).astype(jnp.int32)
    slot = jnp.where(group <= 0, -1, group * rows + rank)
    slot_ids = lax.broadcasted_iota(jnp.int32, (groups * rows, width), 0)
    chooser = (slot_ids == slot).astype(jnp.float32).astype(jnp.bfloat16)
    choose_ref[...] = chooser
    loads[1].wait()
    middle = sol_points // 2
    pad_ref[:, :sol_points] = sol_ref[...]
    solution = pad_ref[...]
    loads[2].wait()
    trace_ref[...] = (
        table_dot(centred(solution, sol_points), spread_ref) + solution[:, middle : middle + 1]
    )
    blocks = to_faces(tile_reader(trace_ref, elements), elements, face_points, list(range(FIELDS)))
    for face, block in enumerate(blocks):
        face_ref[face * elements : (face + 1) * elements] = block
    store_message(pick_rows(chooser, face_ref[...]), msg_refs)


def route_kernel(
    sizes, pad_ref, link_ref, face_ref, grad_ref, grad_traced_ref,
    remote_ref, local_ref, near_ref, slope_ref, traced_ref, row_ref,
):
    elements, sol_points, face_points, dom_count, sub_count, rows = sizes
    faces = 6 * elements
    link = link_row(link_ref, row_ref, elements)
    device, key, side, flip, ahead, back = partner_place(link, elements, dom_count, sub_count)
    mate = flip * sub_count + back
    is_local = (side == 0) & (mate == 0)
    side = jnp.where(side == 0, 0, 3 - side)
    base = jnp.where(is_local, -faces, (side * PAIR * sub_count + mate) * rows)
    lowest = jnp.where(link < 0, -4 * faces, device * faces)
    total = jnp.where(link < 0, -2 * faces, lowest + key)
    width = link.shape[1]
    stack = jnp.concatenate(
        [
            total.astype(jnp.float32),
            lowest.astype(jnp.float32),
            base.astype(jnp.float32),
            jnp.where(is_local, key, -1).astype(jnp.float32),
            jnp.zeros((SUBLANES - 4, width), jnp.float32),
        ],
        axis=0,
    )
    flipped = jnp.transpose(stack)[:faces]
    col = [flipped[:, i : i + 1] for i in range(4)]
    total_row = total.astype(jnp.float32)
    hits = (total_row < col[0]) & (total_row >= col[1])
    rank = jnp.sum(hits.astype(jnp.float32), axis=1, keepdims=True)
    slot = (col[2] + rank).astype(jnp.int32)
    slots = remote_ref.shape[1]
    remote_ref[...] = (lane_ids((faces, slots)) == slot).astype(jnp.float32).astype(jnp.bfloat16)
    local = (lane_ids((faces, width)) == col[3].astype(jnp.int32)).astype(jnp.float32).astype(jnp.bfloat16)
    local_ref[...] = local
    near_ref[...] = pick_rows(local, face_ref[...])
    differ = centred(pad_ref[...], sol_points)
    slope_ref[...] = table_dot(differ, grad_ref)
    traced_ref[...] = table_dot(differ, grad_traced_ref)


def primitive(fields):
    inverse = 1.0 / fields[0]
    velocity = [fields[1 + d] * inverse for d in range(DIRS)]
    kinetic = 0.5 * (fields[1] * velocity[0] + fields[2] * velocity[1] + fields[3] * velocity[2])
    pressure = (heat_ratio - 1.0) * (fields[4] - kinetic)
    return inverse, velocity, pressure


def viscous_terms(fields, inverse, velocity, slopes):
    vel_slope = [
        [(slopes[a][1 + b] - velocity[b] * slopes[a][0]) * inverse for a in range(DIRS)]
        for b in range(DIRS)
    ]
    specific = fields[4] * inverse
    energy_slope = [
        (slopes[a][4] - specific * slopes[a][0]) * inverse
        - (
            velocity[0] * vel_slope[0][a]
            + velocity[1] * vel_slope[1][a]
            + velocity[2] * vel_slope[2][a]
        )
        for a in range(DIRS)
    ]
    divergence = vel_slope[0][0] + vel_slope[1][1] + vel_slope[2][2]
    return vel_slope, energy_slope, divergence


def viscous_flux(velocity, vel_slope, energy_slope, divergence, a):
    stress = []
    for b in range(DIRS):
        member = viscosity * (vel_slope[b][a] + vel_slope[a][b])
        if a == b:
            member = member - 2.0 / 3.0 * viscosity * divergence
        stress.append(member)
    work = velocity[0] * stress[0] + velocity[1] * stress[1] + velocity[2] * stress[2]
    return stress + [work + viscosity * heat_ratio / prandtl * energy_slope[a]]


def field_rows(values, elements, count):
    return [values[k * elements : (k + 1) * elements] for k in range(count)]


def gather_message(parts, scratch_ref, rows, mates):
    mate_refs, first_far, second_far = parts
    scratch_ref[...] = jnp.zeros_like(scratch_ref)
    for index, ref in enumerate(mate_refs):
        scratch_ref[(index + 1) * rows : (index + 2) * rows] = ref[:rows]
    scratch_ref[mates * rows : 2 * mates * rows] = first_far[...]
    scratch_ref[2 * mates * rows : 3 * mates * rows] = second_far[...]
    return scratch_ref[...]


def store_message(message, msg_refs):
    height = message.shape[0] // len(msg_refs)
    for mate, ref in enumerate(msg_refs):
        ref[...] = message[mate * height : (mate + 1) * height]


def normal_viscous(fields, slopes, first, pair):
    def along(values):
        return jnp.where(first, values[pair[0]], values[pair[1]])

    inverse = 1.0 / fields[0]
    velocity = [fields[1 + b] * inverse for b in range(DIRS)]
    speed = along(velocity)
    normal = [along([slopes[a][k] for a in range(DIRS)]) for k in range(FIELDS)]
    own = [normal[1 + b] - velocity[b] * normal[0] for b in range(DIRS)]
    swapped = [
        along([slopes[b][1 + a] for a in range(DIRS)]) - speed * slopes[b][0] for b in range(DIRS)
    ]
    divergence = sum(slopes[a][1 + a] - velocity[a] * slopes[a][0] for a in range(DIRS))
    third = (2.0 / 3.0) * divergence
    scale = viscosity * inverse
    stress = []
    for b in range(DIRS):
        member = own[b] + swapped[b]
        if b in pair:
            here = first if b == pair[0] else jnp.logical_not(first)
            member = member - jnp.where(here, third, 0.0)
        stress.append(scale * member)
    energy = normal[4] - fields[4] * inverse * normal[0]
    energy = energy - (velocity[0] * own[0] + velocity[1] * own[1] + velocity[2] * own[2])
    work = velocity[0] * stress[0] + velocity[1] * stress[1] + velocity[2] * stress[2]
    return stress + [work + (heat_ratio / prandtl) * scale * energy]


def gradient_kernel(sizes, mates, *refs):
    elements, sol_points, face_points, dom_count, sub_count, rows = sizes
    mate_refs = refs[: mates - 1]
    (
        prev_ref, next_ref, remote_ref, near_ref, slope_ref, trace_ref, choose_ref, lift_ref,
    ) = refs[mates - 1 : mates + 7]
    msg_refs = refs[mates + 7 : 2 * mates + 7]
    other_ref, visc_ref, vface_ref, arrived_ref, jump_ref, traced_ref = refs[2 * mates + 7 :]
    arrived = gather_message((mate_refs, prev_ref, next_ref), arrived_ref, rows, mates)
    faces = near_ref[...] + pick_rows(remote_ref[...], arrived)
    for tile in range(2):
        lanes = slice(tile * LANES, (tile + 1) * LANES)
        own = field_rows(trace_ref[:, lanes], elements, FIELDS)
        other = from_faces(faces, list(range(FIELDS)), tile, own, elements, face_points)
        for k in range(FIELDS):
            part = slice(k * elements, (k + 1) * elements)
            other_ref[part, lanes] = other[k]
            jump_ref[part, lanes] = 0.5 * (other[k] - own[k])
    traced_ref[...] = slope_ref[...] + table_dot(jump_ref[...], lift_ref)
    width = 2 * LANES
    chunk = (SUBLANES, LANES)
    for tile in range(2):
        first = first_direction(tile, chunk, face_points)
        sign = side_sign(tile, chunk, face_points)
        lanes = slice(tile * LANES, (tile + 1) * LANES)
        for row in range(0, elements, SUBLANES):
            rows_of = [
                slice(k * elements + row, k * elements + row + SUBLANES) for k in range(FIELDS)
            ]
            fields = [trace_ref[rows_of[k], lanes] for k in range(FIELDS)]
            slopes = []
            for a in range(DIRS):
                start = a * width + tile * LANES
                slopes.append([traced_ref[r, start : start + LANES] for r in rows_of])
            members = normal_viscous(fields, slopes, first, (tile, tile + 1))
            for i in range(4):
                visc_ref[rows_of[i], lanes] = sign * members[i]
    blocks = to_faces(tile_reader(visc_ref, elements), elements, face_points, list(range(1, FIELDS)))
    for face, block in enumerate(blocks):
        vface_ref[face * elements : (face + 1) * elements] = block
    vface_ref[6 * elements :] = jnp.zeros_like(vface_ref[6 * elements :])
    store_message(pick_short(choose_ref[...], vface_ref[...]), msg_refs)


def volume_kernel(
    sizes, pad_ref, slope_ref, trace_ref, other_ref, visc_ref, vface_ref, local_ref,
    lift_ref, normal_ref, div_ref, drop_ref,
    partial_ref, near_ref, flux_ref, jump_ref,
):
    elements, sol_points, face_points, dom_count, sub_count, rows = sizes
    near_ref[...] = pick_short(local_ref[...], vface_ref[...])
    solution = pad_ref[...]
    middle = sol_points // 2
    inside = lane_ids(solution.shape) < sol_points
    solution = jnp.where(inside, solution, solution[:, middle : middle + 1])
    fields = field_rows(solution, elements, FIELDS)
    grad = slope_ref[...] + table_dot(0.5 * (other_ref[...] - trace_ref[...]), lift_ref)
    slopes = [
        field_rows(grad[:, a * LANES : (a + 1) * LANES], elements, FIELDS) for a in range(DIRS)
    ]
    inverse, velocity, pressure = primitive(fields)
    vel_slope, energy_slope, divergence = viscous_terms(fields, inverse, velocity, slopes)
    middles = []
    for a in range(DIRS):
        viscous = viscous_flux(velocity, vel_slope, energy_slope, divergence, a)
        flux = [fields[1 + a]]
        for b in range(DIRS):
            member = fields[1 + b] * velocity[a]
            if a == b:
                member = member + pressure
            flux.append(member - viscous[b])
        flux.append((fields[4] + pressure) * velocity[a] - viscous[3])
        for k in range(FIELDS):
            middles.append(flux[k][:, middle : middle + 1])
            flux_ref[k * elements : (k + 1) * elements, a * LANES : (a + 1) * LANES] = (
                flux[k] - middles[-1]
            )
    flux = flux_ref[...]
    jump_ref[...] = table_dot(flux, normal_ref)
    for tile in range(2):
        shape = (elements, LANES)
        lanes = slice(tile * LANES, (tile + 1) * LANES)
        first = first_direction(tile, shape, face_points)
        sign = side_sign(tile, shape, face_points)
        pair = (tile, tile + 1)
        own = field_rows(trace_ref[:, lanes], elements, FIELDS)
        other = field_rows(other_ref[:, lanes], elements, FIELDS)
        inv_l, vel_l, press_l = primitive(own)
        inv_r, vel_r, press_r = primitive(other)
        speed_l = sign * jnp.where(first, vel_l[pair[0]], vel_l[pair[1]])
        speed_r = sign * jnp.where(first, vel_r[pair[0]], vel_r[pair[1]])
        wave_l = jnp.abs(speed_l) + jnp.sqrt(heat_ratio * press_l * inv_l)
        wave_r = jnp.abs(speed_r) + jnp.sqrt(heat_ratio * press_r * inv_r)
        upwind = 0.5 * jnp.maximum(wave_l, wave_r) + penalty
        press = sign * (press_l + press_r)
        for k in range(FIELDS):
            central = own[k] * speed_l + other[k] * speed_r
            if k == 4:
                central = central + press_l * speed_l + press_r * speed_r
            elif k - 1 == pair[0]:
                central = central + jnp.where(first, press, 0.0)
            elif k - 1 == pair[1]:
                central = central + jnp.where(first, 0.0, press)
            member = 0.5 * central + upwind * (own[k] - other[k])
            if k > 0:
                member = member - 0.5 * visc_ref[(k - 1) * elements : k * elements, lanes]
            level = jnp.where(
                first, middles[pair[0] * FIELDS + k], middles[pair[1] * FIELDS + k]
            )
            part = slice(k * elements, (k + 1) * elements)
            jump_ref[part, lanes] = member - sign * level - jump_ref[part, lanes]
    partial_ref[...] = table_dot(flux, div_ref) + table_dot(jump_ref[...], drop_ref)


def final_kernel(sizes, mates, *refs):
    elements, sol_points, face_points, dom_count, sub_count, rows = sizes
    mate_refs = refs[: mates - 1]
    first_ref, second_ref, remote_ref, near_ref, partial_ref, drop_ref = refs[mates - 1 : mates + 5]
    rate_ref, arrived_ref, visc_ref = refs[mates + 5 :]
    arrived = gather_message((mate_refs, first_ref, second_ref), arrived_ref, rows, mates)
    faces = near_ref[...] + pick_short(remote_ref[...], arrived)
    blank = jnp.zeros((elements, LANES), jnp.float32)
    for tile in range(2):
        members = from_faces(
            faces, list(range(1, FIELDS)), tile, [blank] * (FIELDS - 1), elements, face_points
        )
        for i, member in enumerate(members):
            visc_ref[i * elements : (i + 1) * elements, tile * LANES : (tile + 1) * LANES] = member
    partial = partial_ref[...]
    lifted = table_dot(0.5 * visc_ref[...], drop_ref)
    rate_ref[:elements] = -partial[:elements, :sol_points]
    rate_ref[elements:] = -(partial[elements:] + lifted)[:, :sol_points]


def run_kernel(body, outs, scratch, *operands, space=pltpu.VMEM, limit=16 << 20):
    vmem = pl.BlockSpec(memory_space=pltpu.VMEM)
    if space == pltpu.HBM:
        operands = [pltpu.with_memory_space_constraint(x, pltpu.HBM) for x in operands]
    return pl.pallas_call(
        body,
        out_shape=outs,
        in_specs=[pl.BlockSpec(memory_space=space)] * len(operands),
        out_specs=jax.tree.map(lambda _: vmem, outs),
        scratch_shapes=scratch,
        compiler_params=pltpu.CompilerParams(vmem_limit_bytes=limit),
        cost_estimate=pl.CostEstimate(flops=2 << 30, bytes_accessed=1 << 20, transcendentals=0),
    )(*operands)


def shape_of(shape, dtype=jnp.float32):
    return jax.ShapeDtypeStruct(shape, dtype)


def exchange(blocks, sub_count, dom_count, rows):
    mates = PAIR * sub_count
    arrived = [blocks[0]]
    for mate in range(1, mates):
        flip, shift = divmod(mate, sub_count)
        route = [
            (d * sub_count + s, (d ^ flip) * sub_count + (s + shift) % sub_count)
            for d in range(dom_count)
            for s in range(sub_count)
        ]
        arrived.append(lax.ppermute(blocks[mate], ("dom", "sub"), route))
    far = []
    for side in (1, 2):
        packed = jnp.concatenate([block[side * rows : (side + 1) * rows] for block in arrived])
        hop = PAIR if side == 1 else -PAIR
        route = [(d, (d + hop) % dom_count) for d in range(dom_count)]
        far.append(lax.ppermute(packed, "dom", route))
    return arrived[1:] + far


def shards(solution, face_link):
    spread, grad, lift, normal, div, drop, grad_traced, lift_traced = padded_tables(ORDER + 1)
    sol_points, fields, elements = solution.shape
    face_points = (ORDER + 1) ** 2
    sub_count = lax.axis_size("sub")
    dom_count = lax.axis_size("dom")
    capacity = max(3, elements * 3 // 16)
    rows = -(-capacity // SUBLANES) * SUBLANES
    mates = PAIR * sub_count
    slots = DIRS * mates * rows
    slot_lanes = -(-slots // LANES) * LANES
    faces = 6 * elements
    face_lanes = -(-faces // LANES) * LANES
    sizes = (elements, sol_points, face_points, dom_count, sub_count, rows)
    row_scratch = pltpu.VMEM((1, face_lanes), jnp.int32)
    tall = fields * elements
    width = 2 * LANES
    sol = jnp.transpose(solution, (1, 2, 0)).reshape(tall, sol_points)

    blocks = [shape_of((slots // mates, LANES))] * mates
    *msg, trace, face, choose, padded = run_kernel(
        functools.partial(pack_kernel, sizes),
        (
            *blocks,
            shape_of((tall, width)),
            shape_of((face_lanes, LANES)),
            shape_of((slots, face_lanes), jnp.bfloat16),
            shape_of((tall, LANES)),
        ),
        [
            row_scratch,
            pltpu.VMEM(sol.shape, jnp.float32),
            pltpu.VMEM(face_link.shape, jnp.int32),
            pltpu.VMEM(spread.shape, jnp.bfloat16),
            pltpu.SemaphoreType.DMA((3,)),
        ],
        sol, face_link, spread,
        space=pltpu.HBM,
    )
    pieces = exchange(msg, sub_count, dom_count, rows)
    remote, local, near, slope, traced = run_kernel(
        functools.partial(route_kernel, sizes),
        (
            shape_of((faces, slot_lanes), jnp.bfloat16),
            shape_of((faces, face_lanes), jnp.bfloat16),
            shape_of((faces, LANES)),
            shape_of((tall, DIRS * LANES)),
            shape_of((tall, DIRS * width)),
        ),
        [row_scratch],
        padded, face_link, face, grad, grad_traced,
    )
    *msg, other, visc, vface = run_kernel(
        functools.partial(gradient_kernel, sizes, mates),
        (
            *blocks,
            shape_of((tall, width)),
            shape_of((tall - elements, width)),
            shape_of((face_lanes, LANES)),
        ),
        [
            pltpu.VMEM((slot_lanes, LANES), jnp.float32),
            pltpu.VMEM((tall, width), jnp.float32),
            pltpu.VMEM((tall, DIRS * width), jnp.float32),
        ],
        *pieces, remote, near, traced, trace, choose, lift_traced,
    )
    pieces = exchange(msg, sub_count, dom_count, rows)
    partial, near = run_kernel(
        functools.partial(volume_kernel, sizes),
        (shape_of((tall, LANES)), shape_of((faces, LANES))),
        [
            pltpu.VMEM((tall, DIRS * LANES), jnp.float32),
            pltpu.VMEM((tall, width), jnp.float32),
        ],
        padded, slope, trace, other, visc, vface, local, lift, normal, div, drop,
    )
    rate = run_kernel(
        functools.partial(final_kernel, sizes, mates),
        shape_of((tall, sol_points)),
        [
            pltpu.VMEM((slot_lanes, LANES), jnp.float32),
            pltpu.VMEM((tall - elements, width), jnp.float32),
        ],
        *pieces, remote, near, partial, drop,
    )
    return jnp.transpose(rate.reshape(fields, elements, sol_points), (2, 0, 1))


def solution(mesh):
    in_specs = (P(None, None, ("dom", "sub")), P(None, ("dom", "sub")))
    out_specs = P(None, None, ("dom", "sub"))
    return jax.shard_map(shards, mesh=mesh, in_specs=in_specs, out_specs=out_specs, check_vma=False)
```
